512 devices in a mesh: hel: 16 (over y, x_hi, core), rad: 32 (over z, x_lo).
Axes of the slice: x: 4 (x_hi: 2, x_lo: 2; x = x_hi * 2 + x_lo), y: 4, z: 16, core: 2. Of those that a mesh axis runs over, the one named last changes fastest.
Arguments:
- older_packet: float32 [16, 512, 8, 1024], P('hel', 'rad'), may hold values from -6 to 6
- newer_packet: float32 [16, 512, 8, 1024], P('hel', 'rad'), may hold values from -6 to 6
- kinetic: bfloat16 [512, 512], replicated, may hold values from -1 to 1, as said below
- transform: bfloat16 [16, 1024, 1024], P('hel'), may hold values from -0.1875 to 0.1875
- potential: bfloat16 [512, 8, 1024], P('rad'), may hold values from -2 to 2
- coupling: bfloat16 [16, 1024], P('hel'), may hold values from 0.29882812 to 1.5
- radial_weight: float32 [512], replicated, may hold values from 0.3 to 2
- damping: float32 [512], P('rad'), may hold values from 0.6 to 1
Outputs:
- older_out: float32 [16, 512, 8, 1024], P('hel', 'rad')
- newer_out: float32 [16, 512, 8, 1024], P('hel', 'rad')
The draws below stay inside these ranges and needn't reach their ends.
Inputs may be any that keep to these rules, and one draw needn't show every extreme that they name: kinetic is symmetric.
All inputs are finite; a program needn't handle non-finite values.
Results may differ from the reference program's by a relative error of at most 0.014.
Values may be sent and summed in bfloat16 or wider, within the bound.
No kernel may reach another device: no remote copies, remote signals or barrier semaphores. Data moves between devices by JAX's collectives and lax.ppermute only.
A program may use at most 64 MiB of HBM per device.

```python
import math
import jax
import jax.numpy as jnp
from jax import lax

RADIAL = 512
VIBRATION = 8
ANGULAR = 1024
STEPS = 3
HELICITY = 16


def draw_kinetic(key, part):
    first = jax.random.fold_in(jax.random.fold_in(key, 17), 0)
    noise = jax.random.truncated_normal(first, -4.0, 4.0, (RADIAL, RADIAL), jnp.float32)
    sym = (noise + noise.T) * (0.5 / RADIAL ** 0.5)
    return jnp.clip(sym, -1.0, 1.0).astype(jnp.bfloat16)


def steps_of(own_key, dims, cuts, low, high):
    loudness = 1.0
    for axis_at, blocks in cuts:
        draws = jax.random.uniform(jax.random.fold_in(jax.random.fold_in(own_key, 6), axis_at), (blocks,), jnp.float32, low / len(cuts), high / len(cuts))
        loudness = loudness * jnp.repeat(jnp.exp(draws), dims[axis_at] // blocks).reshape((-1,) + (1,) * (len(dims) - 1 - axis_at))
    return loudness


def bell_draw(key, extent, width, reach, cuts=(), held_as=jnp.bfloat16):
    values = width * jax.random.normal(key, extent, jnp.float32)
    if cuts:
        values = values * steps_of(key, extent, cuts, -0.22, 0.18)
    return jnp.clip(values, -reach, reach).astype(held_as)


def setup_inputs(seed: int = 0) -> dict:
    streams_of = jax.random.split(jax.random.key(seed), 9)
    older_packet = bell_draw(streams_of[0], (HELICITY, RADIAL, VIBRATION, ANGULAR), 1.0, 6.0, ((0, 16), (1, 32)), jnp.float32)
    newer_packet = bell_draw(streams_of[1], (HELICITY, RADIAL, VIBRATION, ANGULAR), 1.0, 6.0, ((0, 16), (1, 32)), jnp.float32)
    kinetic = draw_kinetic(jax.random.fold_in(streams_of[8], 71), 0)
    transform = bell_draw(streams_of[3], (HELICITY, ANGULAR, ANGULAR), ANGULAR ** -0.5, 0.1875, ((0, 16),))
    potential = jnp.clip(jax.random.uniform(streams_of[4], (RADIAL, VIBRATION, ANGULAR), jnp.float32, -2.0, 2.0) * steps_of(streams_of[4], (RADIAL, VIBRATION, ANGULAR), ((0, 32),), -0.4, 0.0), -2.0, 2.0).astype(jnp.bfloat16)
    coupling = jnp.clip(jnp.exp(math.log(1.5) - 1.6133518 * jax.random.uniform(streams_of[5], (HELICITY, ANGULAR), jnp.float32) ** steps_of(streams_of[5], (HELICITY, ANGULAR), ((0, 16),), -0.2, 0.2)), 0.29882812, 1.5).astype(jnp.bfloat16)
    radial_weight = jnp.clip(jnp.exp(jax.random.uniform(streams_of[6], (RADIAL,), jnp.float32, math.log(0.3), math.log(2.0))), 0.3, 2.0)
    damping = jnp.clip(0.6 + 0.39999998 * jax.random.uniform(streams_of[7], (RADIAL,), jnp.float32) ** steps_of(streams_of[7], (RADIAL,), ((0, 32),), -0.2, 0.2), 0.6, 1.0)
    return {"older_packet": older_packet, "newer_packet": newer_packet, "kinetic": kinetic, "transform": transform, "potential": potential, "coupling": coupling, "radial_weight": radial_weight, "damping": damping}


SCALE_FACTOR = 0.35


def angular_block(rounded_block, matrix, potential_flat):
    flat = rounded_block.reshape(RADIAL * VIBRATION, ANGULAR)
    grid = jnp.dot(flat, matrix, preferred_element_type=jnp.float32)
    grid_values = (grid * potential_flat).astype(jnp.bfloat16)
    back = lax.dot_general(grid_values, matrix, (((1,), (1,)), ((), ())), preferred_element_type=jnp.float32)
    return back.reshape(RADIAL, VIBRATION, ANGULAR)


def reference(older_packet, newer_packet, kinetic, transform, potential, coupling, radial_weight, damping):
    kinetic_wide = kinetic.astype(jnp.float32)
    potential_flat = potential.astype(jnp.float32).reshape(RADIAL * VIBRATION, ANGULAR)
    coefficient = coupling.astype(jnp.float32)
    lower_coef = jnp.concatenate([jnp.zeros((1, ANGULAR), jnp.float32), coefficient[:-1]], axis=0)
    damp = damping[None, :, None, None]
    previous = older_packet
    current = newer_packet
    for _ in range(STEPS):
        rounded = current.astype(jnp.bfloat16)
        widened = rounded.astype(jnp.float32)
        radial_part = jnp.einsum("rs,ksva->krva", kinetic_wide, widened)
        empty = jnp.zeros((1, RADIAL, VIBRATION, ANGULAR), jnp.float32)
        below = jnp.concatenate([empty, widened[:-1]], axis=0)
        above = jnp.concatenate([widened[1:], empty], axis=0)
        coriolis_part = radial_weight[None, :, None, None] * (lower_coef[:, None, None, :] * below + coefficient[:, None, None, :] * above)
        off_grid = (radial_part + coriolis_part).astype(jnp.bfloat16)
        off_grid = lax.optimization_barrier(off_grid).astype(jnp.float32)
        angular_part = lax.map(lambda pair: angular_block(pair[0], pair[1], potential_flat), (rounded, transform))
        applied = SCALE_FACTOR * (off_grid + angular_part)
        following = damp * (2.0 * applied - damp * previous)
        previous = current
        current = following
    return previous, current
```

```python
import functools

import jax
import jax.numpy as jnp
from jax import lax
from jax.experimental import pallas as pl
from jax.experimental.pallas import tpu as pltpu
from jax.sharding import PartitionSpec as P

SCALE_FACTOR = 0.35
GAIN = 2.0 * SCALE_FACTOR
F32, BF16 = jnp.float32, jnp.bfloat16


def call(kernel, outs, *args, flops=0):
    shapes = [jax.ShapeDtypeStruct(s, d) for s, d in outs]
    moved = sum(a.size * a.dtype.itemsize for a in args) + sum(s.size * s.dtype.itemsize for s in shapes)
    single = len(shapes) == 1
    return pl.pallas_call(
        kernel,
        out_shape=shapes[0] if single else shapes,
        in_specs=[pl.BlockSpec(memory_space=pltpu.VMEM)] * len(args),
        out_specs=pl.BlockSpec(memory_space=pltpu.VMEM) if single else [pl.BlockSpec(memory_space=pltpu.VMEM)] * len(shapes),
        cost_estimate=pl.CostEstimate(flops=max(flops, 8 * moved), bytes_accessed=moved, transcendentals=0),
        name=kernel.func.__name__ if isinstance(kernel, functools.partial) else kernel.__name__,
    )(*args)


def natural(quarters, piece, width):
    return slice(None), piece // quarters, pl.ds((piece % quarters) * width, width)


def pack(vib, x_ref, o_ref):
    pieces, rows, width = o_ref.shape
    for p in range(pieces):
        o_ref[p] = x_ref[natural(pieces // vib, p, width)].astype(BF16)


def angular(vib, x_ref, t_ref, v_ref, grid_ref, put):
    pieces, rows, width = x_ref.shape
    quarters = pieces // vib
    sources = [
        jnp.concatenate([x_ref[v * quarters + q] for v in range(vib)], axis=0) for q in range(quarters)
    ]
    for g in range(quarters):
        cols = pl.ds(g * width, width)
        total = jnp.zeros((vib * rows, width), F32)
        for q in range(quarters):
            total += jnp.dot(sources[q], t_ref[pl.ds(q * width, width), cols], preferred_element_type=F32)
        grid_ref[:, cols] = (total * v_ref[:, cols].astype(F32)).astype(BF16)
    for q in range(quarters):
        put(q, lax.dot_general(
            grid_ref[...], t_ref[pl.ds(q * width, width), :], (((1,), (1,)), ((), ())), preferred_element_type=F32
        ))


def first_rest(vib, x_ref, t_ref, v_ref, lo_ref, hi_ref, clo_ref, chi_ref, gw_ref, g_ref, dd_ref, old_ref, z_ref, zb_ref, grid_ref):
    pieces, rows, width = x_ref.shape
    quarters = pieces // vib

    def put(q, part):
        for v in range(vib):
            p = v * quarters + q
            mixed = clo_ref[q : q + 1] * lo_ref[p].astype(F32) + chi_ref[q : q + 1] * hi_ref[p].astype(F32)
            old = old_ref[natural(quarters, p, width)]
            z = g_ref[...] * part[v * rows : (v + 1) * rows] + gw_ref[...] * mixed - dd_ref[...] * old
            z_ref[p] = z
            zb_ref[p] = z.astype(BF16)

    angular(vib, x_ref, t_ref, v_ref, grid_ref, put)


def radial(k_ref, x, gall_ref, pieces, put):
    size = k_ref.shape[0]
    rows = size // pieces
    step = 128
    for s in range(0, size, step):
        y = jnp.dot(k_ref[s : s + step], x, preferred_element_type=F32) * gall_ref[s : s + step]
        for i in range(step // rows):
            put(s // rows + i, y[i * rows : (i + 1) * rows])


def first_radial(k_ref, x_ref, gall_ref, zb_ref, kx_ref, out_ref):
    pieces, rows, width = x_ref.shape

    def put(p, y):
        kx_ref[p] = y
        out_ref[p, :rows] = y.astype(BF16)
        out_ref[p, rows:] = zb_ref[p]

    radial(k_ref, x_ref[...].reshape(pieces * rows, width), gall_ref, pieces, put)


def second(vib, r_ref, z_ref, kx_ref, k_ref, gall_ref, t_ref, v_ref, g_ref, dd_ref, new_ref,
           x1_ref, xb_ref, cb_ref, kx1_ref, z1_ref, out_ref, grid_ref):
    pieces, rows, width = z_ref.shape
    quarters = pieces // vib
    for p in range(pieces):
        x = z_ref[p] + r_ref[p, :rows].astype(F32)
        x1_ref[p] = x
        xb_ref[p] = x.astype(BF16)
        cb_ref[p] = (r_ref[p, rows:].astype(F32) + kx_ref[p]).astype(BF16)

    def put_radial(p, y):
        kx1_ref[p] = y
        out_ref[p, :rows] = y.astype(BF16)

    radial(k_ref, cb_ref[...].reshape(pieces * rows, width), gall_ref, pieces, put_radial)

    def put(q, part):
        for v in range(vib):
            p = v * quarters + q
            z = g_ref[...] * part[v * rows : (v + 1) * rows] - dd_ref[...] * new_ref[natural(quarters, p, width)]
            z1_ref[p] = z
            out_ref[p, rows:] = z.astype(BF16)

    angular(vib, xb_ref, t_ref, v_ref, grid_ref, put)


def third(vib, r_ref, z_ref, kx_ref, lo_ref, hi_ref, clo_ref, chi_ref, gw_ref,
          clow_ref, chiw_ref, cclo_ref, cchi_ref, gwall_ref, k_ref, gall_ref, x2_ref, xb_ref, out_ref, cb_ref):
    pieces, rows, width = z_ref.shape
    quarters = pieces // vib
    for p in range(pieces):
        mixed = cclo_ref[...] * clow_ref[p].astype(F32) + cchi_ref[...] * chiw_ref[p].astype(F32)
        c = r_ref[p, rows:].astype(F32) + kx_ref[p] + gwall_ref[p * rows : (p + 1) * rows] * mixed
        cb_ref[p * rows : (p + 1) * rows] = c.astype(BF16)

    def put_radial(p, y):
        out_ref[p] = y.astype(BF16)

    radial(k_ref, cb_ref[...], gall_ref, pieces, put_radial)
    for p in range(pieces):
        q = p % quarters
        mixed = clo_ref[q : q + 1] * lo_ref[p].astype(F32) + chi_ref[q : q + 1] * hi_ref[p].astype(F32)
        x = z_ref[p] + r_ref[p, :rows].astype(F32) + gw_ref[...] * mixed
        x2_ref[natural(quarters, p, width)] = x
        xb_ref[p] = x.astype(BF16)


def last_rest(vib, x_ref, t_ref, v_ref, g_ref, dd_ref, x1_ref, z_ref, grid_ref):
    pieces, rows, width = x_ref.shape
    quarters = pieces // vib

    def put(q, part):
        for v in range(vib):
            p = v * quarters + q
            z_ref[p] = g_ref[...] * part[v * rows : (v + 1) * rows] - dd_ref[...] * x1_ref[p]

    angular(vib, x_ref, t_ref, v_ref, grid_ref, put)


def last(vib, r_ref, z_ref, lo_ref, hi_ref, clo_ref, chi_ref, gw_ref, x3_ref):
    pieces, rows, width = z_ref.shape
    quarters = pieces // vib
    for p in range(pieces):
        q = p % quarters
        mixed = clo_ref[q : q + 1] * lo_ref[p].astype(F32) + chi_ref[q : q + 1] * hi_ref[p].astype(F32)
        x3_ref[natural(quarters, p, width)] = z_ref[p] + r_ref[p].astype(F32) + gw_ref[...] * mixed


def with_grid(kernel, outs, scratch, *args, flops=0):
    return call(kernel, [*outs, *scratch], *args, flops=flops)[: len(outs)]


def exchange(blocks):
    return lax.all_to_all(blocks, "rad", 0, 0, tiled=True)


def neighbours(array):
    devices = lax.axis_size("hel")
    up = [(i, i + 1) for i in range(devices - 1)]
    return lax.ppermute(array, "hel", up), lax.ppermute(array, "hel", [(j, i) for i, j in up])


def body(older, newer, kinetic, transform, potential, coupling, radial_weight, damping):
    _, rows, vib, ang = newer.shape
    pieces = lax.axis_size("rad")
    quarters = pieces // vib
    width = ang // quarters
    size = rows * pieces
    rank = lax.axis_index("rad")
    flat = (rows * vib, ang)
    packed = (pieces, rows, width)
    double = (pieces, 2 * rows, width)
    old, new = older[0], newer[0]
    table = transform[0]
    pot = jnp.swapaxes(potential, 0, 1).reshape(flat)
    work = [(flat, BF16)]
    k_flops = 2 * size * size * width
    a_flops = 4 * flat[0] * ang * ang

    x0 = call(functools.partial(pack, vib), [(packed, BF16)], new)
    r1 = exchange(x0)
    lo, hi = neighbours(x0)
    coef = coupling.astype(F32)
    below = lax.ppermute(coupling, "hel", [(i, i + 1) for i in range(lax.axis_size("hel") - 1)]).astype(F32)
    all_damp = lax.all_gather(damping, "rad", tiled=True)

    chi, clo = coef.reshape(quarters, width), below.reshape(quarters, width)
    cchi = lax.dynamic_slice_in_dim(coef, (rank % quarters) * width, width, 1)
    cclo = lax.dynamic_slice_in_dim(below, (rank % quarters) * width, width, 1)
    weight = lax.dynamic_slice_in_dim(radial_weight, rank * rows, rows, 0)
    wide = lambda column: jnp.broadcast_to(column[:, None], (rows, width))
    g, gw, dd = wide(GAIN * damping), wide(GAIN * damping * weight), wide(damping * damping)
    gall, gwall = (GAIN * all_damp)[:, None], (GAIN * all_damp * radial_weight)[:, None]

    z0, z0b = with_grid(functools.partial(first_rest, vib), [(packed, F32), (packed, BF16)], work,
                        x0, table, pot, lo, hi, clo, chi, gw, g, dd, old, flops=a_flops)
    kx0, send = call(first_radial, [(packed, F32), (double, BF16)], kinetic, r1, gall, z0b, flops=k_flops)
    r2 = exchange(send)
    x1, x1b, c1b, kx1, z1, send = with_grid(
        functools.partial(second, vib),
        [(packed, F32), (packed, BF16), (packed, BF16), (packed, F32), (packed, F32), (double, BF16)], work,
        r2, z0, kx0, kinetic, gall, table, pot, g, dd, new, flops=a_flops + k_flops)
    r3 = exchange(send)
    lo, hi = neighbours(x1b)
    clow, chiw = neighbours(c1b)
    x2, x2b, send = with_grid(
        functools.partial(third, vib), [(old.shape, F32), (packed, BF16), (packed, BF16)], [((size, width), BF16)],
        r3, z1, kx1, lo, hi, clo, chi, gw, clow, chiw, cclo, cchi, gwall, kinetic, gall, flops=k_flops)
    r4 = exchange(send)
    lo, hi = neighbours(x2b)
    (z2,) = with_grid(functools.partial(last_rest, vib), [(packed, F32)], work, x2b, table, pot, g, dd, x1, flops=a_flops)
    x3 = call(functools.partial(last, vib), [(old.shape, F32)], r4, z2, lo, hi, clo, chi, gw)
    return x2.reshape(newer.shape), x3.reshape(newer.shape)


def solution(mesh):
    return jax.shard_map(
        body,
        mesh=mesh,
        in_specs=(
            P("hel", "rad", None, None),
            P("hel", "rad", None, None),
            P(),
            P("hel", None, None),
            P("rad", None, None),
            P("hel", None),
            P(),
            P("rad"),
        ),
        out_specs=(P("hel", "rad", None, None), P("hel", "rad", None, None)),
        check_vma=False,
    )
```

```python
import functools

import jax
import jax.numpy as jnp
from jax import lax
from jax.experimental import pallas as pl
from jax.experimental.pallas import tpu as pltpu
from jax.sharding import PartitionSpec as P

SCALE_FACTOR = 0.35
GAIN = 2.0 * SCALE_FACTOR
F32, BF16 = jnp.float32, jnp.bfloat16


def call(kernel, outs, *args, flops=0, scalars=(), room=()):
    shapes = [jax.ShapeDtypeStruct(s, d) for s, d in outs]
    moved = sum(a.size * a.dtype.itemsize for a in args) + sum(s.size * s.dtype.itemsize for s in shapes)
    vmem = pl.BlockSpec(memory_space=pltpu.VMEM)
    return pl.pallas_call(
        kernel,
        out_shape=shapes,
        in_specs=[pl.BlockSpec(memory_space=pltpu.SMEM)] * len(scalars) + [vmem] * len(args),
        out_specs=[vmem] * len(shapes),
        scratch_shapes=[pltpu.VMEM(s, d) for s, d in room],
        cost_estimate=pl.CostEstimate(flops=max(flops, 8 * moved), bytes_accessed=moved, transcendentals=0),
        name=kernel.func.__name__,
    )(*scalars, *args)


def natural(quarters, piece, width):
    return slice(None), piece // quarters, pl.ds((piece % quarters) * width, width)


def column(values, shape):
    row = lax.broadcasted_iota(jnp.int32, shape, 0)
    out = jnp.full(shape, values[0], F32)
    for i, value in enumerate(values[1:], 1):
        out = jnp.where(row == i, value, out)
    return out


def own_columns(rows, width, rank_ref, d_ref, w_ref):
    damp = [d_ref[i] for i in range(rows)]
    weight = [w_ref[rank_ref[0] * rows + i] for i in range(rows)]
    d = column(damp, (rows, width))
    return GAIN * d, GAIN * d * column(weight, (rows, width)), d * d


def pack(vib, d_ref, x_ref, c_ref, sent_ref, x0_ref):
    pieces, rows, width = x0_ref.shape
    pieces -= 1
    quarters, half = pieces // vib, width // 2
    for p in range(pieces):
        x = x_ref[natural(quarters, p, width)].astype(BF16)
        x0_ref[p] = x
        sent_ref[p, :rows] = x[:, :half]
        sent_ref[p, rows : 2 * rows] = x[:, half:]
    c = c_ref[...].astype(F32)
    x0_ref[pieces] = column([c[:, q * width : (q + 1) * width] for q in range(quarters)], (rows, width)).astype(BF16)
    tile = (rows // 2, half)
    lane = lax.broadcasted_iota(jnp.int32, tile, 1)
    fine = [column([d_ref[h * rows // 2 + i] for i in range(rows // 2)], tile) for h in range(2)]
    high = [f.astype(BF16).astype(F32) for f in fine]
    low = [f - h for f, h in zip(fine, high)]
    mixed = jnp.where(lane < half // 2, jnp.where(lane < half // 4, high[0], low[0]), jnp.where(lane < 3 * half // 4, high[1], low[1]))
    for p in range(pieces):
        sent_ref[p, 2 * rows :] = mixed.astype(BF16)


def angular(vib, x_ref, t_ref, v_ref, grid_ref, put):
    rows, width = x_ref.shape[1:]
    quarters = t_ref.shape[0] // width
    sources = [
        jnp.concatenate([x_ref[v * quarters + q] for v in range(vib)], axis=0) for q in range(quarters)
    ]
    for g in range(quarters):
        cols = pl.ds(g * width, width)
        total = jnp.zeros((vib * rows, width), F32)
        for q in range(quarters):
            total += jnp.dot(sources[q], t_ref[pl.ds(q * width, width), cols], preferred_element_type=F32)
        grid_ref[:, cols] = (total * v_ref[:, cols].astype(F32)).astype(BF16)
    for q in range(quarters):
        put(q, lax.dot_general(
            grid_ref[...], t_ref[pl.ds(q * width, width), :], (((1,), (1,)), ((), ())), preferred_element_type=F32
        ))


def mixer(lo_ref, hi_ref, below_ref, c_ref, rows, width):
    pieces = lo_ref.shape[0]
    quarters = c_ref.shape[1] // width
    clo = below_ref[below_ref.shape[0] - 1].astype(F32)
    below = [jnp.broadcast_to(clo[q : q + 1], (rows, width)) for q in range(quarters)]
    own = [jnp.broadcast_to(c_ref[:, q * width : (q + 1) * width].astype(F32), (rows, width)) for q in range(quarters)]

    def mixed(p, q=None, lo=lo_ref, hi=hi_ref):
        q = p % quarters if q is None else q
        if isinstance(q, int):
            return below[q] * lo[p].astype(F32) + own[q] * hi[p].astype(F32)
        under, over = below[0], own[0]
        for i in range(1, quarters):
            under, over = jnp.where(q == i, below[i], under), jnp.where(q == i, own[i], over)
        return under * lo[p].astype(F32) + over * hi[p].astype(F32)

    return mixed


def first_rest(vib, rank_ref, d_ref, w_ref, x_ref, t_ref, v_ref, lo_ref, hi_ref, c_ref, old_ref, z_ref, zb_ref, wall_ref, grid_ref):
    pieces, rows, width = z_ref.shape
    quarters = pieces // vib
    g, gw, dd = own_columns(rows, width, rank_ref, d_ref, w_ref)
    mixed = mixer(lo_ref, hi_ref, lo_ref, c_ref, rows, width)
    for p in range(pieces):
        wall_ref[p] = column([w_ref[p * rows + i] for i in range(rows)], wall_ref.shape[1:])

    def put(q, part):
        for v in range(vib):
            p = v * quarters + q
            z = g * part[v * rows : (v + 1) * rows] + gw * mixed(p) - dd * old_ref[natural(quarters, p, width)]
            z_ref[p] = z
            zb_ref[p] = z.astype(BF16)

    angular(vib, x_ref, t_ref, v_ref, grid_ref, put)


def radial(k_ref, x, gall_ref, put):
    pieces, rows, _ = gall_ref.shape
    step = 128 // rows
    for s in range(0, pieces, step):
        y = jnp.dot(k_ref[s * rows : (s + step) * rows], x, preferred_element_type=F32)
        for i in range(step):
            g = gall_ref[s + i]
            put(s + i, y[i * rows : (i + 1) * rows] * jnp.concatenate([g, g], axis=1))


def first_radial(k_ref, r_ref, zb_ref, kx_ref, gall_ref, out_ref, x_ref):
    pieces, rows, width = zb_ref.shape
    half = width // 2
    for p in range(pieces):
        at = slice(p * rows, (p + 1) * rows)
        x_ref[at, :half] = r_ref[p, :rows]
        x_ref[at, half:] = r_ref[p, rows : 2 * rows]
        tile = r_ref[p, 2 * rows :].astype(F32)
        for h in range(2):
            lane = h * half // 2
            d = tile[:, lane : lane + 1] + tile[:, lane + half // 4 : lane + half // 4 + 1]
            gall_ref[p, h * rows // 2 : (h + 1) * rows // 2] = jnp.broadcast_to(GAIN * d, (rows // 2, half))

    def put(p, y):
        kx_ref[p] = y
        out_ref[p, :rows] = y.astype(BF16)
        out_ref[p, rows:] = zb_ref[p]

    radial(k_ref, x_ref[...], gall_ref, put)


def second(vib, rank_ref, d_ref, w_ref, r_ref, z_ref, kx_ref, k_ref, gall_ref, t_ref, v_ref, new_ref,
           x1_ref, xb_ref, cb_ref, kx1_ref, z1_ref, out_ref, grid_ref):
    pieces, rows, width = z_ref.shape
    quarters = pieces // vib
    g, _, dd = own_columns(rows, width, rank_ref, d_ref, w_ref)
    for p in range(pieces):
        x = z_ref[p] + r_ref[p, :rows].astype(F32)
        x1_ref[p] = x
        xb_ref[p] = x.astype(BF16)
        cb_ref[p] = (r_ref[p, rows:].astype(F32) + kx_ref[p]).astype(BF16)

    def put_radial(p, y):
        kx1_ref[p] = y
        out_ref[p, :rows] = y.astype(BF16)

    radial(k_ref, cb_ref[...].reshape(pieces * rows, width), gall_ref, put_radial)

    def put(q, part):
        for v in range(vib):
            p = v * quarters + q
            z = g * part[v * rows : (v + 1) * rows] - dd * new_ref[natural(quarters, p, width)]
            z1_ref[p] = z
            out_ref[p, rows:] = z.astype(BF16)

    angular(vib, xb_ref, t_ref, v_ref, grid_ref, put)


def third(vib, rank_ref, d_ref, w_ref, r_ref, z_ref, kx_ref, lo_ref, hi_ref, low_ref, hiw_ref, below_ref, c_ref,
          wall_ref, k_ref, gall_ref, x2_ref, xb_ref, out_ref, cb_ref):
    pieces, rows, width = z_ref.shape
    quarters = pieces // vib
    _, gw, _ = own_columns(rows, width, rank_ref, d_ref, w_ref)
    mixed = mixer(lo_ref, hi_ref, below_ref, c_ref, rows, width)
    own = lax.rem(rank_ref[0], quarters)
    for p in range(pieces):
        gwall = gall_ref[p] * wall_ref[p]
        gwall = jnp.concatenate([gwall, gwall], axis=1)
        c = r_ref[p, rows:].astype(F32) + kx_ref[p] + gwall * mixed(p, own, low_ref, hiw_ref)
        cb_ref[p * rows : (p + 1) * rows] = c.astype(BF16)

    def put_radial(p, y):
        out_ref[p] = y.astype(BF16)

    radial(k_ref, cb_ref[...], gall_ref, put_radial)
    for p in range(pieces):
        x = z_ref[p] + r_ref[p, :rows].astype(F32) + gw * mixed(p)
        x2_ref[natural(quarters, p, width)] = x
        xb_ref[p] = x.astype(BF16)


def last_rest(vib, rank_ref, d_ref, w_ref, x_ref, t_ref, v_ref, x1_ref, z_ref, grid_ref):
    pieces, rows, width = x_ref.shape
    quarters = pieces // vib
    g, _, dd = own_columns(rows, width, rank_ref, d_ref, w_ref)

    def put(q, part):
        for v in range(vib):
            p = v * quarters + q
            z_ref[p] = g * part[v * rows : (v + 1) * rows] - dd * x1_ref[p]

    angular(vib, x_ref, t_ref, v_ref, grid_ref, put)


def last(vib, rank_ref, d_ref, w_ref, r_ref, z_ref, lo_ref, hi_ref, below_ref, c_ref, x3_ref):
    pieces, rows, width = z_ref.shape
    quarters = pieces // vib
    _, gw, _ = own_columns(rows, width, rank_ref, d_ref, w_ref)
    mixed = mixer(lo_ref, hi_ref, below_ref, c_ref, rows, width)
    for p in range(pieces):
        x3_ref[natural(quarters, p, width)] = z_ref[p] + r_ref[p].astype(F32) + gw * mixed(p)


def exchange(blocks):
    return lax.all_to_all(blocks, "rad", 0, 0, tiled=True)


def neighbours(array):
    devices = lax.axis_size("hel")
    up = [(i, i + 1) for i in range(devices - 1)]
    return lax.ppermute(array, "hel", up), lax.ppermute(array, "hel", [(j, i) for i, j in up])


def body(older, newer, kinetic, transform, potential, coupling, radial_weight, damping):
    _, rows, vib, ang = newer.shape
    pieces = lax.axis_size("rad")
    width = ang // (pieces // vib)
    size = rows * pieces
    flat = (rows * vib, ang)
    packed, double = (pieces, rows, width), (pieces, 2 * rows, width)
    old, new = older[0], newer[0]
    table = transform[0]
    pot = jnp.swapaxes(potential, 0, 1).reshape(flat)
    own = (lax.axis_index("rad").astype(jnp.int32).reshape(1), damping, radial_weight)
    grid = (flat, BF16)
    k_flops = 2 * size * size * width
    a_flops = 4 * flat[0] * ang * ang
    part = lambda kernel: functools.partial(kernel, vib)

    sent, x0 = call(
        part(pack), [((pieces, 5 * rows // 2, width // 2), BF16), ((pieces + 1, rows, width), BF16)],
        new, coupling, scalars=(damping,))
    r1 = exchange(sent)
    lo, hi = neighbours(x0)
    below = lo
    z0, z0b, wall = call(
        part(first_rest), [(packed, F32), (packed, BF16), ((pieces, rows, width // 2), F32)],
        x0, table, pot, lo, hi, coupling, old, scalars=own, room=[grid], flops=a_flops)
    kx0, gall, sent = call(
        functools.partial(first_radial), [(packed, F32), ((pieces, rows, width // 2), F32), (double, BF16)],
        kinetic, r1, z0b, room=[((size, width), BF16)], flops=k_flops)
    r2 = exchange(sent)
    x1, x1b, c1b, kx1, z1, sent = call(
        part(second), [(packed, F32), (packed, BF16), (packed, BF16), (packed, F32), (packed, F32), (double, BF16)],
        r2, z0, kx0, kinetic, gall, table, pot, new, scalars=own, room=[grid], flops=a_flops + k_flops)
    r3 = exchange(sent)
    lo, hi = neighbours(x1b)
    low, hiw = neighbours(c1b)
    x2, x2b, sent = call(
        part(third), [(old.shape, F32), (packed, BF16), (packed, BF16)],
        r3, z1, kx1, lo, hi, low, hiw, below, coupling, wall, kinetic, gall,
        scalars=own, room=[((size, width), BF16)], flops=k_flops)
    r4 = exchange(sent)
    lo, hi = neighbours(x2b)
    (z2,) = call(part(last_rest), [(packed, F32)], x2b, table, pot, x1, scalars=own, room=[grid], flops=a_flops)
    (x3,) = call(part(last), [(old.shape, F32)], r4, z2, lo, hi, below, coupling, scalars=own)
    return x2.reshape(newer.shape), x3.reshape(newer.shape)


def solution(mesh):
    return jax.shard_map(
        body,
        mesh=mesh,
        in_specs=(
            P("hel", "rad", None, None),
            P("hel", "rad", None, None),
            P(),
            P("hel", None, None),
            P("rad", None, None),
            P("hel", None),
            P(),
            P("rad"),
        ),
        out_specs=(P("hel", "rad", None, None), P("hel", "rad", None, None)),
        check_vma=False,
    )
```

```python
import functools

import jax
import jax.numpy as jnp
from jax import lax
from jax.experimental import pallas as pl
from jax.experimental.pallas import tpu as pltpu
from jax.sharding import PartitionSpec as P

SCALE_FACTOR = 0.35
GAIN = 2.0 * SCALE_FACTOR
F32, BF16 = jnp.float32, jnp.bfloat16
GRANT = 10 * 2**20


def call(kernel, outs, *args, flops=0, scalars=(), room=(), grant=None):
    shapes = [jax.ShapeDtypeStruct(s, d) for s, d in outs]
    moved = sum(a.size * a.dtype.itemsize for a in args) + sum(s.size * s.dtype.itemsize for s in shapes)
    vmem = pl.BlockSpec(memory_space=pltpu.VMEM)
    return pl.pallas_call(
        kernel,
        out_shape=shapes,
        in_specs=[pl.BlockSpec(memory_space=pltpu.SMEM)] * len(scalars) + [vmem] * len(args),
        out_specs=[vmem] * len(shapes),
        scratch_shapes=[pltpu.VMEM(s, d) for s, d in room],
        compiler_params=pltpu.CompilerParams(vmem_limit_bytes=grant),
        cost_estimate=pl.CostEstimate(flops=max(flops, 8 * moved), bytes_accessed=moved, transcendentals=0),
        name=kernel.func.__name__,
    )(*scalars, *args)


def natural(quarters, piece, width):
    return slice(None), piece // quarters, pl.ds((piece % quarters) * width, width)


def column(values, shape):
    row = lax.broadcasted_iota(jnp.int32, shape, 0)
    out = jnp.full(shape, values[0], F32)
    for i, value in enumerate(values[1:], 1):
        out = jnp.where(row == i, value, out)
    return out


def own_columns(rows, width, rank_ref, d_ref, w_ref):
    damp = [d_ref[i] for i in range(rows)]
    weight = [w_ref[rank_ref[0] * rows + i] for i in range(rows)]
    d = column(damp, (rows, width))
    return GAIN * d, GAIN * d * column(weight, (rows, width)), d * d


def pack(vib, d_ref, x_ref, c_ref, sent_ref, x0_ref):
    pieces, rows, width = x0_ref.shape
    pieces -= 1
    quarters, half = pieces // vib, width // 2
    for p in range(pieces):
        x = x_ref[natural(quarters, p, width)].astype(BF16)
        x0_ref[p] = x
        sent_ref[p, :rows] = x[:, :half]
        sent_ref[p, rows : 2 * rows] = x[:, half:]
    c = c_ref[...].astype(F32)
    x0_ref[pieces] = column([c[:, q * width : (q + 1) * width] for q in range(quarters)], (rows, width)).astype(BF16)
    tile = (rows // 2, half)
    lane = lax.broadcasted_iota(jnp.int32, tile, 1)
    fine = [column([d_ref[h * rows // 2 + i] for i in range(rows // 2)], tile) for h in range(2)]
    high = [f.astype(BF16).astype(F32) for f in fine]
    low = [f - h for f, h in zip(fine, high)]
    mixed = jnp.where(lane < half // 2, jnp.where(lane < half // 4, high[0], low[0]), jnp.where(lane < 3 * half // 4, high[1], low[1]))
    for p in range(pieces):
        sent_ref[p, 2 * rows :] = mixed.astype(BF16)


def angular(vib, x_ref, t_ref, v_ref, grid_ref, put):
    rows, width = x_ref.shape[1:]
    quarters = t_ref.shape[0] // width
    sources = [
        jnp.concatenate([x_ref[v * quarters + q] for v in range(vib)], axis=0) for q in range(quarters)
    ]
    for g in range(quarters):
        cols = pl.ds(g * width, width)
        total = jnp.zeros((vib * rows, width), F32)
        for q in range(quarters):
            total += jnp.dot(sources[q], t_ref[pl.ds(q * width, width), cols], preferred_element_type=F32)
        grid_ref[:, cols] = (total * v_ref[:, cols].astype(F32)).astype(BF16)
    for q in range(quarters):
        put(q, lax.dot_general(
            grid_ref[...], t_ref[pl.ds(q * width, width), :], (((1,), (1,)), ((), ())), preferred_element_type=F32
        ))


def mixed(consts_ref, p, quarters, lo_ref, hi_ref):
    q = p % quarters
    return consts_ref[5 + q] * lo_ref[p].astype(F32) + consts_ref[5 + quarters + q] * hi_ref[p].astype(F32)


def first_rest(vib, rank_ref, d_ref, w_ref, x_ref, t_ref, v_ref, lo_ref, hi_ref, c_ref, old_ref, z_ref, wall_ref, consts_ref, grid_ref):
    pieces, rows, width = z_ref.shape
    quarters = pieces // vib
    tile = (rows, width)
    g, gw, dd = own_columns(rows, width, rank_ref, d_ref, w_ref)
    consts_ref[0], consts_ref[1], consts_ref[2] = g, gw, dd
    below = lo_ref[pieces].astype(F32)
    own = lax.rem(rank_ref[0], quarters)
    under, over = jnp.zeros(tile, F32), jnp.zeros(tile, F32)
    for q in range(quarters):
        lower = jnp.broadcast_to(below[q : q + 1], tile)
        upper = jnp.broadcast_to(c_ref[:, q * width : (q + 1) * width].astype(F32), tile)
        consts_ref[5 + q], consts_ref[5 + quarters + q] = lower, upper
        under, over = jnp.where(own == q, lower, under), jnp.where(own == q, upper, over)
    consts_ref[3], consts_ref[4] = under, over
    for p in range(pieces):
        wall_ref[p] = column([w_ref[p * rows + i] for i in range(rows)], wall_ref.shape[1:])

    def put(q, part):
        for v in range(vib):
            p = v * quarters + q
            z = g * part[v * rows : (v + 1) * rows] + gw * mixed(consts_ref, p, quarters, lo_ref, hi_ref)
            z_ref[p] = (z - dd * old_ref[natural(quarters, p, width)]).astype(BF16)

    angular(vib, x_ref, t_ref, v_ref, grid_ref, put)


def radial(k_ref, x, pieces, put):
    rows = k_ref.shape[0] // pieces
    step = 128 // rows
    for s in range(0, pieces, step):
        y = jnp.dot(k_ref[s * rows : (s + step) * rows], x, preferred_element_type=F32)
        for i in range(step):
            put(s + i, y[i * rows : (i + 1) * rows])


def twice(half):
    return jnp.concatenate([half, half], axis=1)


def first_radial(k_ref, r_ref, z_ref, gall_ref, out_ref, x_ref):
    pieces, rows, width = z_ref.shape
    half = width // 2
    for p in range(pieces):
        at = slice(p * rows, (p + 1) * rows)
        x_ref[at, :half] = r_ref[p, :rows]
        x_ref[at, half:] = r_ref[p, rows : 2 * rows]
        tile = r_ref[p, 2 * rows :].astype(F32)
        for h in range(2):
            lane = h * half // 2
            d = tile[:, lane : lane + 1] + tile[:, lane + half // 4 : lane + half // 4 + 1]
            gall_ref[p, h * rows // 2 : (h + 1) * rows // 2] = jnp.broadcast_to(GAIN * d, (rows // 2, half))

    def put(p, y):
        out_ref[p, :rows] = (y * twice(gall_ref[p])).astype(BF16)
        out_ref[p, rows:] = z_ref[p]

    radial(k_ref, x_ref[...], pieces, put)


def second(vib, r_ref, s_ref, k_ref, gall_ref, wall_ref, t_ref, v_ref, x0_ref, consts_ref,
           xb_ref, cb_ref, out_ref, gwall_ref, grid_ref):
    pieces, rows, width = xb_ref.shape
    gwall_ref[...] = gall_ref[...] * wall_ref[...]
    quarters = pieces // vib
    g, dd = consts_ref[0], consts_ref[2]
    for p in range(pieces):
        xb_ref[p] = (s_ref[p, rows:].astype(F32) + r_ref[p, :rows].astype(F32)).astype(BF16)
        cb_ref[p] = (r_ref[p, rows:].astype(F32) + s_ref[p, :rows].astype(F32)).astype(BF16)

    def put_radial(p, y):
        out_ref[p, :rows] = (y * twice(gall_ref[p])).astype(BF16)

    radial(k_ref, cb_ref[...].reshape(pieces * rows, width), pieces, put_radial)

    def put(q, part):
        for v in range(vib):
            p = v * quarters + q
            out_ref[p, rows:] = (g * part[v * rows : (v + 1) * rows] - dd * x0_ref[p].astype(F32)).astype(BF16)

    angular(vib, xb_ref, t_ref, v_ref, grid_ref, put)


def third_columns(r_ref, s_ref, lo_ref, hi_ref, consts_ref, gwall_ref, k_ref, out_ref, cb_ref):
    pieces, rows, _ = out_ref.shape
    for p in range(pieces):
        mix = consts_ref[3] * lo_ref[p].astype(F32) + consts_ref[4] * hi_ref[p].astype(F32)
        c = r_ref[p, rows:].astype(F32) + s_ref[p, :rows].astype(F32) + twice(gwall_ref[p]) * mix
        cb_ref[p * rows : (p + 1) * rows] = c.astype(BF16)

    def put(p, y):
        out_ref[p] = y.astype(BF16)

    radial(k_ref, cb_ref[...], pieces, put)


def third_rows(vib, r_ref, s_ref, lo_ref, hi_ref, consts_ref, x2_ref, xb_ref):
    pieces, rows, width = xb_ref.shape
    quarters = pieces // vib
    for p in range(pieces):
        x = s_ref[p, rows:].astype(F32) + r_ref[p, :rows].astype(F32)
        x = x + consts_ref[1] * mixed(consts_ref, p, quarters, lo_ref, hi_ref)
        x2_ref[natural(quarters, p, width)] = x
        xb_ref[p] = x.astype(BF16)


def last_rest(vib, x_ref, t_ref, v_ref, x1_ref, consts_ref, z_ref, grid_ref):
    pieces, rows, width = x_ref.shape
    quarters = pieces // vib

    def put(q, part):
        for v in range(vib):
            p = v * quarters + q
            z_ref[p] = consts_ref[0] * part[v * rows : (v + 1) * rows] - consts_ref[2] * x1_ref[p].astype(F32)

    angular(vib, x_ref, t_ref, v_ref, grid_ref, put)


def last(vib, r_ref, z_ref, lo_ref, hi_ref, consts_ref, x3_ref):
    pieces, rows, width = z_ref.shape
    quarters = pieces // vib
    for p in range(pieces):
        x = z_ref[p] + consts_ref[0] * r_ref[p].astype(F32) + consts_ref[1] * mixed(consts_ref, p, quarters, lo_ref, hi_ref)
        x3_ref[natural(quarters, p, width)] = x


def exchange(blocks):
    return lax.all_to_all(blocks, "rad", 0, 0, tiled=True)


def neighbours(array):
    devices = lax.axis_size("hel")
    up = [(i, i + 1) for i in range(devices - 1)]
    return lax.ppermute(array, "hel", up), lax.ppermute(array, "hel", [(j, i) for i, j in up])


def body(older, newer, kinetic, transform, potential, coupling, radial_weight, damping):
    _, rows, vib, ang = newer.shape
    pieces = lax.axis_size("rad")
    width = ang // (pieces // vib)
    size = rows * pieces
    flat = (rows * vib, ang)
    packed, double = (pieces, rows, width), (pieces, 2 * rows, width)
    old, new = older[0], newer[0]
    table = transform[0]
    pot = jnp.swapaxes(potential, 0, 1).reshape(flat)
    own = (lax.axis_index("rad").astype(jnp.int32).reshape(1), damping, radial_weight)
    grid = (flat, BF16)
    k_flops = 2 * size * size * width
    a_flops = 4 * flat[0] * ang * ang
    part = lambda kernel: functools.partial(kernel, vib)

    sent, x0 = call(
        part(pack), [((pieces, 5 * rows // 2, width // 2), BF16), ((pieces + 1, rows, width), BF16)],
        new, coupling, scalars=(damping,))
    r1 = exchange(sent)
    lo, hi = neighbours(x0)
    quarters = pieces // vib
    z0, wall, consts = call(
        part(first_rest), [(packed, BF16), ((pieces, rows, width // 2), F32), ((5 + 2 * quarters, rows, width), F32)],
        x0, table, pot, lo, hi, coupling, old, scalars=own, room=[grid], flops=a_flops)
    gall, sent = call(
        functools.partial(first_radial), [((pieces, rows, width // 2), F32), (double, BF16)],
        kinetic, r1, z0, room=[((size, width), BF16)], flops=k_flops, grant=GRANT)
    r2 = exchange(sent)
    x1, c1, sent, gwall = call(
        part(second), [(packed, BF16), (packed, BF16), (double, BF16), (gall.shape, F32)],
        r2, sent, kinetic, gall, wall, table, pot, x0, consts, room=[grid], flops=a_flops + k_flops, grant=GRANT)
    r3 = exchange(sent)
    lo, hi = neighbours(x1)
    low, hiw = neighbours(c1)
    r3, lo, hi = lax.optimization_barrier((r3, lo, hi))
    (sent4,) = call(
        functools.partial(third_columns), [(packed, BF16)],
        r3, sent, low, hiw, consts, gwall, kinetic, room=[((size, width), BF16)], flops=k_flops, grant=GRANT)
    r4 = exchange(sent4)
    x2, x2b = call(part(third_rows), [(old.shape, F32), (packed, BF16)], r3, sent, lo, hi, consts, grant=GRANT)
    lo, hi = neighbours(x2b)
    (z2,) = call(part(last_rest), [(packed, F32)], x2b, table, pot, x1, consts, room=[grid], flops=a_flops)
    (x3,) = call(part(last), [(old.shape, F32)], r4, z2, lo, hi, consts, grant=GRANT)
    return x2.reshape(newer.shape), x3.reshape(newer.shape)


def solution(mesh):
    return jax.shard_map(
        body,
        mesh=mesh,
        in_specs=(
            P("hel", "rad", None, None),
            P("hel", "rad", None, None),
            P(),
            P("hel", None, None),
            P("rad", None, None),
            P("hel", None),
            P(),
            P("rad"),
        ),
        out_specs=(P("hel", "rad", None, None), P("hel", "rad", None, None)),
        check_vma=False,
    )
```

```python
import functools

import jax
import jax.numpy as jnp
from jax import lax
from jax.experimental import pallas as pl
from jax.experimental.pallas import tpu as pltpu
from jax.sharding import PartitionSpec as P

SCALE_FACTOR = 0.35
GAIN = 2.0 * SCALE_FACTOR
F32, BF16 = jnp.float32, jnp.bfloat16
GRANT = 10 * 2**20


def call(kernel, outs, *args, flops=0, scalars=(), room=(), grant=None):
    shapes = [jax.ShapeDtypeStruct(s, d) for s, d in outs]
    moved = sum(a.size * a.dtype.itemsize for a in args) + sum(s.size * s.dtype.itemsize for s in shapes)
    vmem = pl.BlockSpec(memory_space=pltpu.VMEM)
    return pl.pallas_call(
        kernel,
        out_shape=shapes,
        in_specs=[pl.BlockSpec(memory_space=pltpu.SMEM)] * len(scalars) + [vmem] * len(args),
        out_specs=[vmem] * len(shapes),
        scratch_shapes=[pltpu.VMEM(s, d) for s, d in room],
        compiler_params=pltpu.CompilerParams(vmem_limit_bytes=grant),
        cost_estimate=pl.CostEstimate(flops=max(flops, 8 * moved), bytes_accessed=moved, transcendentals=0),
        name=kernel.func.__name__,
    )(*scalars, *args)


def natural(quarters, piece, width):
    return slice(None), piece // quarters, pl.ds((piece % quarters) * width, width)


def column(values, shape):
    row = lax.broadcasted_iota(jnp.int32, shape, 0)
    out = jnp.full(shape, values[0], F32)
    for i, value in enumerate(values[1:], 1):
        out = jnp.where(row == i, value, out)
    return out


def own_columns(rows, width, rank_ref, d_ref, w_ref):
    damp = [d_ref[i] for i in range(rows)]
    weight = [w_ref[rank_ref[0] * rows + i] for i in range(rows)]
    d = column(damp, (rows, width))
    return GAIN * d, GAIN * d * column(weight, (rows, width)), d * d


def pack(vib, d_ref, x_ref, c_ref, sent_ref, x0_ref):
    pieces, rows, width = x0_ref.shape
    pieces -= 1
    quarters, half = pieces // vib, width // 2
    for p in range(pieces):
        x = x_ref[natural(quarters, p, width)].astype(BF16)
        x0_ref[p] = x
        sent_ref[p, :rows] = x[:, :half]
        sent_ref[p, rows : 2 * rows] = x[:, half:]
    c = c_ref[...].astype(F32)
    x0_ref[pieces] = column([c[:, q * width : (q + 1) * width] for q in range(quarters)], (rows, width)).astype(BF16)
    tile = (rows // 2, half)
    lane = lax.broadcasted_iota(jnp.int32, tile, 1)
    fine = [column([d_ref[h * rows // 2 + i] for i in range(rows // 2)], tile) for h in range(2)]
    high = [f.astype(BF16).astype(F32) for f in fine]
    low = [f - h for f, h in zip(fine, high)]
    mixed = jnp.where(lane < half // 2, jnp.where(lane < half // 4, high[0], low[0]), jnp.where(lane < 3 * half // 4, high[1], low[1]))
    for p in range(pieces):
        sent_ref[p, 2 * rows :] = mixed.astype(BF16)


def angular(vib, x_ref, t_ref, v_ref, grid_ref, put):
    rows, width = x_ref.shape[1:]
    quarters = t_ref.shape[0] // width
    sources = [
        jnp.concatenate([x_ref[v * quarters + q] for v in range(vib)], axis=0) for q in range(quarters)
    ]
    for g in range(quarters):
        cols = pl.ds(g * width, width)
        total = jnp.zeros((vib * rows, width), F32)
        for q in range(quarters):
            total += jnp.dot(sources[q], t_ref[pl.ds(q * width, width), cols], preferred_element_type=F32)
        grid_ref[:, cols] = (total * v_ref[:, cols].astype(F32)).astype(BF16)
    for q in range(quarters):
        put(q, lax.dot_general(
            grid_ref[...], t_ref[pl.ds(q * width, width), :], (((1,), (1,)), ((), ())), preferred_element_type=F32
        ))


def mixed(consts_ref, p, quarters, lo_ref, hi_ref):
    q = p % quarters
    return consts_ref[5 + q] * lo_ref[p].astype(F32) + consts_ref[5 + quarters + q] * hi_ref[p].astype(F32)


def first_angular(vib, rank_ref, d_ref, w_ref, x_ref, t_ref, v_ref, old_ref, z_ref, wall_ref, rows_ref, grid_ref):
    pieces, rows, width = z_ref.shape
    quarters = pieces // vib
    g, gw, dd = own_columns(rows, width, rank_ref, d_ref, w_ref)
    rows_ref[0], rows_ref[1], rows_ref[2] = g, gw, dd
    for p in range(pieces):
        wall_ref[p] = column([w_ref[p * rows + i] for i in range(rows)], wall_ref.shape[1:])

    def put(q, part):
        for v in range(vib):
            p = v * quarters + q
            z_ref[p] = g * part[v * rows : (v + 1) * rows] - dd * old_ref[natural(quarters, p, width)]

    angular(vib, x_ref, t_ref, v_ref, grid_ref, put)


def first_coriolis(vib, rank_ref, za_ref, lo_ref, hi_ref, c_ref, rows_ref, z_ref, consts_ref):
    pieces, rows, width = z_ref.shape
    quarters = pieces // vib
    tile = (rows, width)
    below = lo_ref[pieces].astype(F32)
    own = lax.rem(rank_ref[0], quarters)
    under, over = jnp.zeros(tile, F32), jnp.zeros(tile, F32)
    for q in range(quarters):
        lower = jnp.broadcast_to(below[q : q + 1], tile)
        upper = jnp.broadcast_to(c_ref[:, q * width : (q + 1) * width].astype(F32), tile)
        consts_ref[5 + q], consts_ref[5 + quarters + q] = lower, upper
        under, over = jnp.where(own == q, lower, under), jnp.where(own == q, upper, over)
    for i in range(3):
        consts_ref[i] = rows_ref[i]
    consts_ref[3], consts_ref[4] = under, over
    for p in range(pieces):
        z_ref[p] = (za_ref[p] + consts_ref[1] * mixed(consts_ref, p, quarters, lo_ref, hi_ref)).astype(BF16)


def radial(k_ref, x, pieces, put):
    rows = k_ref.shape[0] // pieces
    step = 128 // rows
    for s in range(0, pieces, step):
        y = jnp.dot(k_ref[s * rows : (s + step) * rows], x, preferred_element_type=F32)
        for i in range(step):
            put(s + i, y[i * rows : (i + 1) * rows])


def twice(half):
    return jnp.concatenate([half, half], axis=1)


def first_radial(k_ref, r_ref, z_ref, gall_ref, out_ref, x_ref):
    pieces, rows, width = z_ref.shape
    half = width // 2
    for p in range(pieces):
        at = slice(p * rows, (p + 1) * rows)
        x_ref[at, :half] = r_ref[p, :rows]
        x_ref[at, half:] = r_ref[p, rows : 2 * rows]
        tile = r_ref[p, 2 * rows :].astype(F32)
        for h in range(2):
            lane = h * half // 2
            d = tile[:, lane : lane + 1] + tile[:, lane + half // 4 : lane + half // 4 + 1]
            gall_ref[p, h * rows // 2 : (h + 1) * rows // 2] = jnp.broadcast_to(GAIN * d, (rows // 2, half))

    def put(p, y):
        out_ref[p, :rows] = (y * twice(gall_ref[p])).astype(BF16)
        out_ref[p, rows:] = z_ref[p]

    radial(k_ref, x_ref[...], pieces, put)


def second(vib, r_ref, s_ref, k_ref, gall_ref, wall_ref, t_ref, v_ref, x0_ref, consts_ref,
           xb_ref, cw_ref, out_ref, cb_ref, grid_ref):
    pieces, rows, width = xb_ref.shape
    quarters = pieces // vib
    g, dd = consts_ref[0], consts_ref[2]
    for p in range(pieces):
        xb_ref[p] = (s_ref[p, rows:].astype(F32) + r_ref[p, :rows].astype(F32)).astype(BF16)
        c = r_ref[p, rows:].astype(F32) + s_ref[p, :rows].astype(F32)
        cb_ref[p * rows : (p + 1) * rows] = c.astype(BF16)
        cw_ref[p] = (twice(gall_ref[p] * wall_ref[p]) * c).astype(BF16)

    def put_radial(p, y):
        out_ref[p, :rows] = (y * twice(gall_ref[p])).astype(BF16)

    radial(k_ref, cb_ref[...], pieces, put_radial)

    def put(q, part):
        for v in range(vib):
            p = v * quarters + q
            out_ref[p, rows:] = (g * part[v * rows : (v + 1) * rows] - dd * x0_ref[p].astype(F32)).astype(BF16)

    angular(vib, xb_ref, t_ref, v_ref, grid_ref, put)


def third_columns(r_ref, s_ref, lo_ref, hi_ref, consts_ref, k_ref, out_ref, cb_ref):
    pieces, rows, _ = out_ref.shape
    for p in range(pieces):
        mix = consts_ref[3] * lo_ref[p].astype(F32) + consts_ref[4] * hi_ref[p].astype(F32)
        c = r_ref[p, rows:].astype(F32) + s_ref[p, :rows].astype(F32) + mix
        cb_ref[p * rows : (p + 1) * rows] = c.astype(BF16)

    def put(p, y):
        out_ref[p] = y.astype(BF16)

    radial(k_ref, cb_ref[...], pieces, put)


def third_rows(vib, r_ref, s_ref, lo_ref, hi_ref, consts_ref, x2_ref, xb_ref):
    pieces, rows, width = xb_ref.shape
    quarters = pieces // vib
    for p in range(pieces):
        x = s_ref[p, rows:].astype(F32) + r_ref[p, :rows].astype(F32)
        x = x + consts_ref[1] * mixed(consts_ref, p, quarters, lo_ref, hi_ref)
        x2_ref[natural(quarters, p, width)] = x
        xb_ref[p] = x.astype(BF16)


def last_rest(vib, x_ref, t_ref, v_ref, x1_ref, consts_ref, z_ref, grid_ref):
    pieces, rows, width = x_ref.shape
    quarters = pieces // vib

    def put(q, part):
        for v in range(vib):
            p = v * quarters + q
            z_ref[p] = consts_ref[0] * part[v * rows : (v + 1) * rows] - consts_ref[2] * x1_ref[p].astype(F32)

    angular(vib, x_ref, t_ref, v_ref, grid_ref, put)


def last(vib, r_ref, z_ref, lo_ref, hi_ref, consts_ref, x3_ref):
    pieces, rows, width = z_ref.shape
    quarters = pieces // vib
    for p in range(pieces):
        x = z_ref[p] + consts_ref[0] * r_ref[p].astype(F32) + consts_ref[1] * mixed(consts_ref, p, quarters, lo_ref, hi_ref)
        x3_ref[natural(quarters, p, width)] = x


def exchange(blocks):
    return lax.all_to_all(blocks, "rad", 0, 0, tiled=True)


def neighbours(array):
    devices = lax.axis_size("hel")
    up = [(i, i + 1) for i in range(devices - 1)]
    return lax.ppermute(array, "hel", up), lax.ppermute(array, "hel", [(j, i) for i, j in up])


def body(older, newer, kinetic, transform, potential, coupling, radial_weight, damping):
    _, rows, vib, ang = newer.shape
    pieces = lax.axis_size("rad")
    width = ang // (pieces // vib)
    size = rows * pieces
    flat = (rows * vib, ang)
    packed, double = (pieces, rows, width), (pieces, 2 * rows, width)
    old, new = older[0], newer[0]
    table = transform[0]
    pot = jnp.swapaxes(potential, 0, 1).reshape(flat)
    own = (lax.axis_index("rad").astype(jnp.int32).reshape(1), damping, radial_weight)
    grid = (flat, BF16)
    k_flops = 2 * size * size * width
    a_flops = 4 * flat[0] * ang * ang
    part = lambda kernel: functools.partial(kernel, vib)

    sent, x0 = call(
        part(pack), [((pieces, 5 * rows // 2, width // 2), BF16), ((pieces + 1, rows, width), BF16)],
        new, coupling, scalars=(damping,))
    r1 = exchange(sent)
    lo, hi = neighbours(x0)
    quarters = pieces // vib
    za, wall, own_rows = call(
        part(first_angular), [(packed, F32), ((pieces, rows, width // 2), F32), ((3, rows, width), F32)],
        x0, table, pot, old, scalars=own, room=[grid], flops=a_flops)
    z0, consts = call(
        part(first_coriolis), [(packed, BF16), ((5 + 2 * quarters, rows, width), F32)],
        za, lo, hi, coupling, own_rows, scalars=own[:1])
    gall, sent = call(
        functools.partial(first_radial), [((pieces, rows, width // 2), F32), (double, BF16)],
        kinetic, r1, z0, room=[((size, width), BF16)], flops=k_flops, grant=GRANT)
    r2 = exchange(sent)
    x1, c1, sent = call(
        part(second), [(packed, BF16), (packed, BF16), (double, BF16)],
        r2, sent, kinetic, gall, wall, table, pot, x0, consts, room=[((size, width), BF16), grid], flops=a_flops + k_flops, grant=GRANT)
    r3 = exchange(sent)
    lo, hi = neighbours(x1)
    low, hiw = neighbours(c1)
    r3, lo, hi = lax.optimization_barrier((r3, lo, hi))
    (sent4,) = call(
        functools.partial(third_columns), [(packed, BF16)],
        r3, sent, low, hiw, consts, kinetic, room=[((size, width), BF16)], flops=k_flops, grant=GRANT)
    r4 = exchange(sent4)
    x2, x2b = call(part(third_rows), [(old.shape, F32), (packed, BF16)], r3, sent, lo, hi, consts, grant=GRANT)
    lo, hi = neighbours(x2b)
    (z2,) = call(part(last_rest), [(packed, F32)], x2b, table, pot, x1, consts, room=[grid], flops=a_flops)
    (x3,) = call(part(last), [(old.shape, F32)], r4, z2, lo, hi, consts, grant=GRANT)
    return x2.reshape(newer.shape), x3.reshape(newer.shape)


def solution(mesh):
    return jax.shard_map(
        body,
        mesh=mesh,
        in_specs=(
            P("hel", "rad", None, None),
            P("hel", "rad", None, None),
            P(),
            P("hel", None, None),
            P("rad", None, None),
            P("hel", None),
            P(),
            P("rad"),
        ),
        out_specs=(P("hel", "rad", None, None), P("hel", "rad", None, None)),
        check_vma=False,
    )
```

```python
import functools

import jax
import jax.numpy as jnp
from jax import lax
from jax.experimental import pallas as pl
from jax.experimental.pallas import tpu as pltpu
from jax.sharding import PartitionSpec as P

SCALE_FACTOR = 0.35
GAIN = 2.0 * SCALE_FACTOR
F32, BF16 = jnp.float32, jnp.bfloat16
GRANT = 10 * 2**20


def call(kernel, outs, *args, flops=0, scalars=(), room=(), grant=None):
    shapes = [jax.ShapeDtypeStruct(s, d) for s, d in outs]
    moved = sum(a.size * a.dtype.itemsize for a in args) + sum(s.size * s.dtype.itemsize for s in shapes)
    vmem = pl.BlockSpec(memory_space=pltpu.VMEM)
    return pl.pallas_call(
        kernel,
        out_shape=shapes,
        in_specs=[pl.BlockSpec(memory_space=pltpu.SMEM)] * len(scalars) + [vmem] * len(args),
        out_specs=[vmem] * len(shapes),
        scratch_shapes=[pltpu.VMEM(s, d) for s, d in room],
        compiler_params=pltpu.CompilerParams(vmem_limit_bytes=grant),
        cost_estimate=pl.CostEstimate(flops=max(flops, 8 * moved), bytes_accessed=moved, transcendentals=0),
        name=kernel.func.__name__,
    )(*scalars, *args)


def natural(quarters, piece, width):
    return slice(None), piece // quarters, pl.ds((piece % quarters) * width, width)


def column(values, shape):
    row = lax.broadcasted_iota(jnp.int32, shape, 0)
    out = jnp.full(shape, values[0], F32)
    for i, value in enumerate(values[1:], 1):
        out = jnp.where(row == i, value, out)
    return out


def own_columns(rows, width, rank_ref, d_ref, w_ref):
    damp = [d_ref[i] for i in range(rows)]
    weight = [w_ref[rank_ref[0] * rows + i] for i in range(rows)]
    d = column(damp, (rows, width))
    return GAIN * d, GAIN * d * column(weight, (rows, width)), d * d


def pack(vib, d_ref, x_ref, c_ref, sent_ref, x0_ref):
    pieces, rows, width = x0_ref.shape
    pieces -= 1
    quarters, half = pieces // vib, width // 2
    for p in range(pieces):
        for h in range(2):
            first = (p % quarters * 2 + h) * vib + p // quarters
            x = x_ref[pl.ds(first, rows, stride=2 * quarters * vib), :].astype(BF16)
            x0_ref[p, :, h * half : (h + 1) * half] = x
            sent_ref[p, h * rows : (h + 1) * rows] = x
    c = c_ref[...].astype(F32)
    x0_ref[pieces] = column([c[:, q * width : (q + 1) * width] for q in range(quarters)], (rows, width)).astype(BF16)
    tile = (rows // 2, half)
    lane = lax.broadcasted_iota(jnp.int32, tile, 1)
    fine = [column([d_ref[h * rows // 2 + i] for i in range(rows // 2)], tile) for h in range(2)]
    high = [f.astype(BF16).astype(F32) for f in fine]
    low = [f - h for f, h in zip(fine, high)]
    mixed = jnp.where(lane < half // 2, jnp.where(lane < half // 4, high[0], low[0]), jnp.where(lane < 3 * half // 4, high[1], low[1]))
    for p in range(pieces):
        sent_ref[p, 2 * rows :] = mixed.astype(BF16)


def angular(vib, x_ref, t_ref, v_ref, grid_ref, put):
    rows, width = x_ref.shape[1:]
    quarters = t_ref.shape[0] // width
    sources = [
        jnp.concatenate([x_ref[v * quarters + q] for v in range(vib)], axis=0) for q in range(quarters)
    ]
    for g in range(quarters):
        cols = pl.ds(g * width, width)
        total = jnp.zeros((vib * rows, width), F32)
        for q in range(quarters):
            total += jnp.dot(sources[q], t_ref[pl.ds(q * width, width), cols], preferred_element_type=F32)
        grid_ref[:, cols] = (total * v_ref[:, cols].astype(F32)).astype(BF16)
    for q in range(quarters):
        put(q, lax.dot_general(
            grid_ref[...], t_ref[pl.ds(q * width, width), :], (((1,), (1,)), ((), ())), preferred_element_type=F32
        ))


def mixed(consts_ref, p, quarters, lo_ref, hi_ref):
    q = p % quarters
    return consts_ref[5 + q] * lo_ref[p].astype(F32) + consts_ref[5 + quarters + q] * hi_ref[p].astype(F32)


def first_angular(vib, rank_ref, d_ref, w_ref, x_ref, t_ref, v_ref, old_ref, z_ref, wall_ref, rows_ref, grid_ref):
    pieces, rows, width = z_ref.shape
    quarters = pieces // vib
    g, gw, dd = own_columns(rows, width, rank_ref, d_ref, w_ref)
    rows_ref[0], rows_ref[1], rows_ref[2] = g, gw, dd
    for p in range(pieces):
        wall_ref[p] = column([w_ref[p * rows + i] for i in range(rows)], wall_ref.shape[1:])

    def put(q, part):
        for v in range(vib):
            p = v * quarters + q
            z_ref[p] = g * part[v * rows : (v + 1) * rows] - dd * old_ref[natural(quarters, p, width)]

    angular(vib, x_ref, t_ref, v_ref, grid_ref, put)


def first_coriolis(vib, rank_ref, za_ref, lo_ref, hi_ref, c_ref, rows_ref, z_ref, consts_ref):
    pieces, rows, width = z_ref.shape
    quarters = pieces // vib
    tile = (rows, width)
    below = lo_ref[pieces].astype(F32)
    own = lax.rem(rank_ref[0], quarters)
    under, over = jnp.zeros(tile, F32), jnp.zeros(tile, F32)
    for q in range(quarters):
        lower = jnp.broadcast_to(below[q : q + 1], tile)
        upper = jnp.broadcast_to(c_ref[:, q * width : (q + 1) * width].astype(F32), tile)
        consts_ref[5 + q], consts_ref[5 + quarters + q] = lower, upper
        under, over = jnp.where(own == q, lower, under), jnp.where(own == q, upper, over)
    for i in range(3):
        consts_ref[i] = rows_ref[i]
    consts_ref[3], consts_ref[4] = under, over
    for p in range(pieces):
        z_ref[p] = (za_ref[p] + consts_ref[1] * mixed(consts_ref, p, quarters, lo_ref, hi_ref)).astype(BF16)


def radial(k_ref, x, pieces, put):
    rows = k_ref.shape[0] // pieces
    step = 128 // rows
    for s in range(0, pieces, step):
        y = jnp.dot(k_ref[s * rows : (s + step) * rows], x, preferred_element_type=F32)
        for i in range(step):
            put(s + i, y[i * rows : (i + 1) * rows])


def twice(half):
    return jnp.concatenate([half, half], axis=1)


def first_radial(k_ref, r_ref, z_ref, gall_ref, out_ref, x_ref):
    pieces, rows, width = z_ref.shape
    half = width // 2
    for p in range(pieces):
        at = slice(p * rows, (p + 1) * rows)
        x_ref[at, :half] = r_ref[p, :rows]
        x_ref[at, half:] = r_ref[p, rows : 2 * rows]
        tile = r_ref[p, 2 * rows :].astype(F32)
        for h in range(2):
            lane = h * half // 2
            d = tile[:, lane : lane + 1] + tile[:, lane + half // 4 : lane + half // 4 + 1]
            gall_ref[p, h * rows // 2 : (h + 1) * rows // 2] = jnp.broadcast_to(GAIN * d, (rows // 2, half))

    def put(p, y):
        out_ref[p, :rows] = (y * twice(gall_ref[p])).astype(BF16)
        out_ref[p, rows:] = z_ref[p]

    radial(k_ref, x_ref[...], pieces, put)


def second(vib, r_ref, s_ref, k_ref, gall_ref, wall_ref, t_ref, v_ref, x0_ref, consts_ref,
           xb_ref, cw_ref, out_ref, cb_ref, grid_ref):
    pieces, rows, width = xb_ref.shape
    quarters = pieces // vib
    g, dd = consts_ref[0], consts_ref[2]
    for p in range(pieces):
        xb_ref[p] = (s_ref[p, rows:].astype(F32) + r_ref[p, :rows].astype(F32)).astype(BF16)
        c = r_ref[p, rows:].astype(F32) + s_ref[p, :rows].astype(F32)
        cb_ref[p * rows : (p + 1) * rows] = c.astype(BF16)
        cw_ref[p] = (twice(gall_ref[p] * wall_ref[p]) * c).astype(BF16)

    def put_radial(p, y):
        out_ref[p, :rows] = (y * twice(gall_ref[p])).astype(BF16)

    radial(k_ref, cb_ref[...], pieces, put_radial)

    def put(q, part):
        for v in range(vib):
            p = v * quarters + q
            out_ref[p, rows:] = (g * part[v * rows : (v + 1) * rows] - dd * x0_ref[p].astype(F32)).astype(BF16)

    angular(vib, xb_ref, t_ref, v_ref, grid_ref, put)


def third_ahead(vib, s_ref, lo_ref, hi_ref, low_ref, hiw_ref, consts_ref, zr_ref, zc_ref):
    pieces, rows, width = zr_ref.shape
    quarters = pieces // vib
    for p in range(pieces):
        mix = mixed(consts_ref, p, quarters, lo_ref, hi_ref)
        zr_ref[p] = (s_ref[p, rows:].astype(F32) + consts_ref[1] * mix).astype(BF16)
        mix = consts_ref[3] * low_ref[p].astype(F32) + consts_ref[4] * hiw_ref[p].astype(F32)
        zc_ref[p] = (s_ref[p, :rows].astype(F32) + mix).astype(BF16)


def third_columns(r_ref, z_ref, k_ref, out_ref, cb_ref):
    pieces, rows, _ = out_ref.shape
    for p in range(pieces):
        cb_ref[p * rows : (p + 1) * rows] = (r_ref[p, rows:].astype(F32) + z_ref[p].astype(F32)).astype(BF16)

    def put(p, y):
        out_ref[p] = y.astype(BF16)

    radial(k_ref, cb_ref[...], pieces, put)


def third_rows(vib, r_ref, z_ref, x2_ref, xb_ref):
    pieces, rows, width = xb_ref.shape
    for p in range(pieces):
        x = z_ref[p].astype(F32) + r_ref[p, :rows].astype(F32)
        x2_ref[natural(pieces // vib, p, width)] = x
        xb_ref[p] = x.astype(BF16)


def last_rest(vib, x_ref, t_ref, v_ref, x1_ref, consts_ref, z_ref, grid_ref):
    pieces, rows, width = x_ref.shape
    quarters = pieces // vib

    def put(q, part):
        for v in range(vib):
            p = v * quarters + q
            z_ref[p] = consts_ref[0] * part[v * rows : (v + 1) * rows] - consts_ref[2] * x1_ref[p].astype(F32)

    angular(vib, x_ref, t_ref, v_ref, grid_ref, put)


def last(vib, r_ref, z_ref, lo_ref, hi_ref, consts_ref, x3_ref):
    pieces, rows, width = z_ref.shape
    quarters = pieces // vib
    for p in range(pieces):
        x = z_ref[p] + consts_ref[0] * r_ref[p].astype(F32) + consts_ref[1] * mixed(consts_ref, p, quarters, lo_ref, hi_ref)
        x3_ref[natural(quarters, p, width)] = x


def exchange(blocks):
    return lax.all_to_all(blocks, "rad", 0, 0, tiled=True)


def neighbours(array):
    devices = lax.axis_size("hel")
    up = [(i, i + 1) for i in range(devices - 1)]
    return lax.ppermute(array, "hel", up), lax.ppermute(array, "hel", [(j, i) for i, j in up])


def body(older, newer, kinetic, transform, potential, coupling, radial_weight, damping):
    _, rows, vib, ang = newer.shape
    pieces = lax.axis_size("rad")
    width = ang // (pieces // vib)
    size = rows * pieces
    flat = (rows * vib, ang)
    packed, double = (pieces, rows, width), (pieces, 2 * rows, width)
    old = older[0]
    tiles = newer.reshape(rows, vib, -1, width // 2).transpose(0, 2, 1, 3).reshape(-1, width // 2)
    table = transform[0]
    pot = jnp.swapaxes(potential, 0, 1).reshape(flat)
    own = (lax.axis_index("rad").astype(jnp.int32).reshape(1), damping, radial_weight)
    grid = (flat, BF16)
    k_flops = 2 * size * size * width
    a_flops = 4 * flat[0] * ang * ang
    part = lambda kernel: functools.partial(kernel, vib)

    sent, x0 = call(
        part(pack), [((pieces, 5 * rows // 2, width // 2), BF16), ((pieces + 1, rows, width), BF16)],
        tiles, coupling, scalars=(damping,))
    r1 = exchange(sent)
    lo, hi = neighbours(x0)
    quarters = pieces // vib
    za, wall, own_rows = call(
        part(first_angular), [(packed, F32), ((pieces, rows, width // 2), F32), ((3, rows, width), F32)],
        x0, table, pot, old, scalars=own, room=[grid], flops=a_flops)
    z0, consts = call(
        part(first_coriolis), [(packed, BF16), ((5 + 2 * quarters, rows, width), F32)],
        za, lo, hi, coupling, own_rows, scalars=own[:1])
    gall, sent = call(
        functools.partial(first_radial), [((pieces, rows, width // 2), F32), (double, BF16)],
        kinetic, r1, z0, room=[((size, width), BF16)], flops=k_flops, grant=GRANT)
    r2 = exchange(sent)
    x1, c1, sent = call(
        part(second), [(packed, BF16), (packed, BF16), (double, BF16)],
        r2, sent, kinetic, gall, wall, table, pot, x0, consts, room=[((size, width), BF16), grid], flops=a_flops + k_flops, grant=GRANT)
    r3 = exchange(sent)
    lo, hi = neighbours(x1)
    low, hiw = neighbours(c1)
    zr, zc = call(
        part(third_ahead), [(packed, BF16), (packed, BF16)], sent, lo, hi, low, hiw, consts, grant=GRANT)
    r3, zr, zc = lax.optimization_barrier((r3, zr, zc))
    (sent4,) = call(
        functools.partial(third_columns), [(packed, BF16)],
        r3, zc, kinetic, room=[((size, width), BF16)], flops=k_flops, grant=GRANT)
    r4 = exchange(sent4)
    x2, x2b = call(part(third_rows), [(old.shape, F32), (packed, BF16)], r3, zr, grant=GRANT)
    lo, hi = neighbours(x2b)
    (z2,) = call(part(last_rest), [(packed, F32)], x2b, table, pot, x1, consts, room=[grid], flops=a_flops)
    (x3,) = call(part(last), [(old.shape, F32)], r4, z2, lo, hi, consts, grant=GRANT)
    return x2.reshape(newer.shape), x3.reshape(newer.shape)


def solution(mesh):
    return jax.shard_map(
        body,
        mesh=mesh,
        in_specs=(
            P("hel", "rad", None, None),
            P("hel", "rad", None, None),
            P(),
            P("hel", None, None),
            P("rad", None, None),
            P("hel", None),
            P(),
            P("rad"),
        ),
        out_specs=(P("hel", "rad", None, None), P("hel", "rad", None, None)),
        check_vma=False,
    )
```

```python
import functools

import jax
import jax.numpy as jnp
from jax import lax
from jax.experimental import pallas as pl
from jax.experimental.pallas import tpu as pltpu
from jax.sharding import PartitionSpec as P

SCALE_FACTOR = 0.35
GAIN = 2.0 * SCALE_FACTOR
F32, BF16 = jnp.float32, jnp.bfloat16
GRANT = 10 * 2**20


def call(kernel, outs, *args, flops=0, scalars=(), room=(), grant=None):
    shapes = [jax.ShapeDtypeStruct(s, d) for s, d in outs]
    moved = sum(a.size * a.dtype.itemsize for a in args) + sum(s.size * s.dtype.itemsize for s in shapes)
    vmem = pl.BlockSpec(memory_space=pltpu.VMEM)
    return pl.pallas_call(
        kernel,
        out_shape=shapes,
        in_specs=[pl.BlockSpec(memory_space=pltpu.SMEM)] * len(scalars) + [vmem] * len(args),
        out_specs=[vmem] * len(shapes),
        scratch_shapes=[pltpu.VMEM(s, d) for s, d in room],
        compiler_params=pltpu.CompilerParams(vmem_limit_bytes=grant),
        cost_estimate=pl.CostEstimate(flops=max(flops, 8 * moved), bytes_accessed=moved, transcendentals=0),
        name=kernel.func.__name__,
    )(*scalars, *args)


def natural(quarters, piece, width):
    return slice(None), piece // quarters, pl.ds((piece % quarters) * width, width)


def column(values, shape):
    row = lax.broadcasted_iota(jnp.int32, shape, 0)
    out = jnp.full(shape, values[0], F32)
    for i, value in enumerate(values[1:], 1):
        out = jnp.where(row == i, value, out)
    return out


def own_columns(rows, width, rank_ref, d_ref, w_ref):
    damp = [d_ref[i] for i in range(rows)]
    weight = [w_ref[rank_ref[0] * rows + i] for i in range(rows)]
    d = column(damp, (rows, width))
    return GAIN * d, GAIN * d * column(weight, (rows, width)), d * d


def pack(vib, d_ref, x_ref, c_ref, sent_ref, x0_ref):
    pieces, rows, width = x0_ref.shape
    pieces -= 1
    quarters, half = pieces // vib, width // 2
    for p in range(pieces):
        for h in range(2):
            first = (p % quarters * 2 + h) * vib + p // quarters
            x = x_ref[pl.ds(first, rows, stride=2 * quarters * vib), :].astype(BF16)
            x0_ref[p, :, h * half : (h + 1) * half] = x
            sent_ref[p, h * rows : (h + 1) * rows] = x
    c = c_ref[...].astype(F32)
    x0_ref[pieces] = column([c[:, q * width : (q + 1) * width] for q in range(quarters)], (rows, width)).astype(BF16)
    tile = (rows // 2, half)
    lane = lax.broadcasted_iota(jnp.int32, tile, 1)
    fine = [column([d_ref[h * rows // 2 + i] for i in range(rows // 2)], tile) for h in range(2)]
    high = [f.astype(BF16).astype(F32) for f in fine]
    low = [f - h for f, h in zip(fine, high)]
    mixed = jnp.where(lane < half // 2, jnp.where(lane < half // 4, high[0], low[0]), jnp.where(lane < 3 * half // 4, high[1], low[1]))
    for p in range(pieces):
        sent_ref[p, 2 * rows :] = mixed.astype(BF16)


def angular(vib, x_ref, t_ref, v_ref, grid_ref, put):
    rows, width = x_ref.shape[1:]
    quarters = t_ref.shape[0] // width
    sources = [
        jnp.concatenate([x_ref[v * quarters + q] for v in range(vib)], axis=0) for q in range(quarters)
    ]
    for g in range(quarters):
        cols = pl.ds(g * width, width)
        total = jnp.zeros((vib * rows, width), F32)
        for q in range(quarters):
            total += jnp.dot(sources[q], t_ref[pl.ds(q * width, width), cols], preferred_element_type=F32)
        grid_ref[:, cols] = (total * v_ref[:, cols].astype(F32)).astype(BF16)
    for q in range(quarters):
        put(q, lax.dot_general(
            grid_ref[...], t_ref[pl.ds(q * width, width), :], (((1,), (1,)), ((), ())), preferred_element_type=F32
        ))


def mixed(consts_ref, p, quarters, lo_ref, hi_ref):
    q = p % quarters
    return consts_ref[5 + q] * lo_ref[p].astype(F32) + consts_ref[5 + quarters + q] * hi_ref[p].astype(F32)


def first_angular(vib, rank_ref, d_ref, w_ref, x_ref, t_ref, v_ref, old_ref, z_ref, wall_ref, rows_ref, grid_ref):
    pieces, rows, width = z_ref.shape
    quarters = pieces // vib
    g, gw, dd = own_columns(rows, width, rank_ref, d_ref, w_ref)
    rows_ref[0], rows_ref[1], rows_ref[2] = g, gw, dd
    for p in range(pieces):
        wall_ref[p] = column([w_ref[p * rows + i] for i in range(rows)], wall_ref.shape[1:])

    def put(q, part):
        for v in range(vib):
            p = v * quarters + q
            z_ref[p] = g * part[v * rows : (v + 1) * rows] - dd * old_ref[natural(quarters, p, width)]

    angular(vib, x_ref, t_ref, v_ref, grid_ref, put)


def first_coriolis(vib, rank_ref, za_ref, lo_ref, hi_ref, c_ref, rows_ref, z_ref, consts_ref):
    pieces, rows, width = z_ref.shape
    quarters = pieces // vib
    tile = (rows, width)
    below = lo_ref[pieces].astype(F32)
    own = lax.rem(rank_ref[0], quarters)
    under, over = jnp.zeros(tile, F32), jnp.zeros(tile, F32)
    for q in range(quarters):
        lower = jnp.broadcast_to(below[q : q + 1], tile)
        upper = jnp.broadcast_to(c_ref[:, q * width : (q + 1) * width].astype(F32), tile)
        consts_ref[5 + q], consts_ref[5 + quarters + q] = lower, upper
        under, over = jnp.where(own == q, lower, under), jnp.where(own == q, upper, over)
    for i in range(3):
        consts_ref[i] = rows_ref[i]
    consts_ref[3], consts_ref[4] = under, over
    for p in range(pieces):
        z_ref[p] = (za_ref[p] + consts_ref[1] * mixed(consts_ref, p, quarters, lo_ref, hi_ref)).astype(BF16)


def radial(k_ref, x, pieces, put):
    rows = k_ref.shape[0] // pieces
    step = 128 // rows
    for s in range(0, pieces, step):
        y = jnp.dot(k_ref[s * rows : (s + step) * rows], x, preferred_element_type=F32)
        for i in range(step):
            put(s + i, y[i * rows : (i + 1) * rows])


def twice(half):
    return jnp.concatenate([half, half], axis=1)


def first_radial(k_ref, r_ref, z_ref, gall_ref, out_ref, x_ref):
    pieces, rows, width = z_ref.shape
    half = width // 2
    for p in range(pieces):
        at = slice(p * rows, (p + 1) * rows)
        x_ref[at, :half] = r_ref[p, :rows]
        x_ref[at, half:] = r_ref[p, rows : 2 * rows]
        tile = r_ref[p, 2 * rows :].astype(F32)
        for h in range(2):
            lane = h * half // 2
            d = tile[:, lane : lane + 1] + tile[:, lane + half // 4 : lane + half // 4 + 1]
            gall_ref[p, h * rows // 2 : (h + 1) * rows // 2] = jnp.broadcast_to(GAIN * d, (rows // 2, half))

    def put(p, y):
        out_ref[p, :rows] = (y * twice(gall_ref[p])).astype(BF16)
        out_ref[p, rows:] = z_ref[p]

    radial(k_ref, x_ref[...], pieces, put)


def second(vib, r_ref, s_ref, k_ref, gall_ref, wall_ref, t_ref, v_ref, x0_ref, consts_ref,
           xb_ref, cw_ref, out_ref, cb_ref, grid_ref):
    pieces, rows, width = xb_ref.shape
    quarters = pieces // vib
    g, dd = consts_ref[0], consts_ref[2]
    for p in range(pieces):
        xb_ref[p] = (s_ref[p, rows:].astype(F32) + r_ref[p, :rows].astype(F32)).astype(BF16)
        c = r_ref[p, rows:].astype(F32) + s_ref[p, :rows].astype(F32)
        cb_ref[p * rows : (p + 1) * rows] = c.astype(BF16)
        cw_ref[p] = (twice(gall_ref[p] * wall_ref[p]) * c).astype(BF16)

    def put_radial(p, y):
        out_ref[p, :rows] = (y * twice(gall_ref[p])).astype(BF16)

    radial(k_ref, cb_ref[...], pieces, put_radial)

    def put(q, part):
        for v in range(vib):
            p = v * quarters + q
            out_ref[p, rows:] = (g * part[v * rows : (v + 1) * rows] - dd * x0_ref[p].astype(F32)).astype(BF16)

    angular(vib, xb_ref, t_ref, v_ref, grid_ref, put)


def third_ahead(vib, s_ref, lo_ref, hi_ref, low_ref, hiw_ref, consts_ref, zr_ref, zc_ref):
    pieces, rows, width = zr_ref.shape
    quarters = pieces // vib
    for p in range(pieces):
        mix = mixed(consts_ref, p, quarters, lo_ref, hi_ref)
        zr_ref[p] = (s_ref[p, rows:].astype(F32) + consts_ref[1] * mix).astype(BF16)
        mix = consts_ref[3] * low_ref[p].astype(F32) + consts_ref[4] * hiw_ref[p].astype(F32)
        zc_ref[p] = (s_ref[p, :rows].astype(F32) + mix).astype(BF16)


def third_columns(r_ref, z_ref, k_ref, out_ref, cb_ref):
    pieces, rows, _ = out_ref.shape
    for p in range(pieces):
        cb_ref[p * rows : (p + 1) * rows] = (r_ref[p, rows:].astype(F32) + z_ref[p].astype(F32)).astype(BF16)

    def put(p, y):
        out_ref[p] = y.astype(BF16)

    radial(k_ref, cb_ref[...], pieces, put)


def third_rows(vib, r_ref, z_ref, x2_ref, xb_ref):
    pieces, rows, width = xb_ref.shape
    for p in range(pieces):
        x = z_ref[p].astype(F32) + r_ref[p, :rows].astype(F32)
        x2_ref[natural(pieces // vib, p, width)] = x
        xb_ref[p] = x.astype(BF16)


def last_rest(vib, x_ref, t_ref, v_ref, x1_ref, consts_ref, z_ref, grid_ref):
    pieces, rows, width = x_ref.shape
    quarters = pieces // vib

    def put(q, part):
        for v in range(vib):
            p = v * quarters + q
            z = consts_ref[0] * part[v * rows : (v + 1) * rows] - consts_ref[2] * x1_ref[p].astype(F32)
            z_ref[p] = z.astype(BF16)

    angular(vib, x_ref, t_ref, v_ref, grid_ref, put)


def last(vib, r_ref, z_ref, lo_ref, hi_ref, consts_ref, x3_ref):
    pieces, rows, width = z_ref.shape
    quarters = pieces // vib
    for p in range(pieces):
        x = z_ref[p].astype(F32) + consts_ref[0] * r_ref[p].astype(F32) + consts_ref[1] * mixed(consts_ref, p, quarters, lo_ref, hi_ref)
        x3_ref[natural(quarters, p, width)] = x


def exchange(blocks):
    return lax.all_to_all(blocks, "rad", 0, 0, tiled=True)


def neighbours(array):
    devices = lax.axis_size("hel")
    up = [(i, i + 1) for i in range(devices - 1)]
    return lax.ppermute(array, "hel", up), lax.ppermute(array, "hel", [(j, i) for i, j in up])


def body(older, newer, kinetic, transform, potential, coupling, radial_weight, damping):
    _, rows, vib, ang = newer.shape
    pieces = lax.axis_size("rad")
    width = ang // (pieces // vib)
    size = rows * pieces
    flat = (rows * vib, ang)
    packed, double = (pieces, rows, width), (pieces, 2 * rows, width)
    old = older[0]
    tiles = newer.reshape(rows, vib, -1, width // 2).transpose(0, 2, 1, 3).reshape(-1, width // 2)
    table = transform[0]
    pot = jnp.swapaxes(potential, 0, 1).reshape(flat)
    own = (lax.axis_index("rad").astype(jnp.int32).reshape(1), damping, radial_weight)
    grid = (flat, BF16)
    k_flops = 2 * size * size * width
    a_flops = 4 * flat[0] * ang * ang
    part = lambda kernel: functools.partial(kernel, vib)

    sent, x0 = call(
        part(pack), [((pieces, 5 * rows // 2, width // 2), BF16), ((pieces + 1, rows, width), BF16)],
        tiles, coupling, scalars=(damping,))
    r1 = exchange(sent)
    lo, hi = neighbours(x0)
    quarters = pieces // vib
    za, wall, own_rows = call(
        part(first_angular), [(packed, F32), ((pieces, rows, width // 2), F32), ((3, rows, width), F32)],
        x0, table, pot, old, scalars=own, room=[grid], flops=a_flops)
    z0, consts = call(
        part(first_coriolis), [(packed, BF16), ((5 + 2 * quarters, rows, width), F32)],
        za, lo, hi, coupling, own_rows, scalars=own[:1])
    gall, sent = call(
        functools.partial(first_radial), [((pieces, rows, width // 2), F32), (double, BF16)],
        kinetic, r1, z0, room=[((size, width), BF16)], flops=k_flops, grant=GRANT)
    r2 = exchange(sent)
    x1, c1, sent = call(
        part(second), [(packed, BF16), (packed, BF16), (double, BF16)],
        r2, sent, kinetic, gall, wall, table, pot, x0, consts, room=[((size, width), BF16), grid], flops=a_flops + k_flops, grant=GRANT)
    r3 = exchange(sent)
    lo, hi = neighbours(x1)
    low, hiw = neighbours(c1)
    zr, zc = call(
        part(third_ahead), [(packed, BF16), (packed, BF16)], sent, lo, hi, low, hiw, consts, grant=GRANT)
    r3, zr, zc = lax.optimization_barrier((r3, zr, zc))
    (sent4,) = call(
        functools.partial(third_columns), [(packed, BF16)],
        r3, zc, kinetic, room=[((size, width), BF16)], flops=k_flops, grant=GRANT)
    r4 = exchange(sent4)
    x2, x2b = call(part(third_rows), [(old.shape, F32), (packed, BF16)], r3, zr, grant=GRANT)
    lo, hi = neighbours(x2b)
    (z2,) = call(part(last_rest), [(packed, BF16)], x2b, table, pot, x1, consts, room=[grid], flops=a_flops)
    (x3,) = call(part(last), [(old.shape, F32)], r4, z2, lo, hi, consts, grant=GRANT)
    return x2.reshape(newer.shape), x3.reshape(newer.shape)


def solution(mesh):
    return jax.shard_map(
        body,
        mesh=mesh,
        in_specs=(
            P("hel", "rad", None, None),
            P("hel", "rad", None, None),
            P(),
            P("hel", None, None),
            P("rad", None, None),
            P("hel", None),
            P(),
            P("rad"),
        ),
        out_specs=(P("hel", "rad", None, None), P("hel", "rad", None, None)),
        check_vma=False,
    )
```
